32 devices in a mesh: grp: 4 (over z), loc: 8 (over y, x, core).
Axes of the slice: x: 2, y: 2, z: 4, core: 2. Of those that a mesh axis runs over, the one named last changes fastest.
Arguments:
- tokens: bfloat16 [4096, 2048], P(('grp', 'loc')), may hold values from -6 to 6
- expert_ids: int32 [4096, 6], P(('grp', 'loc')), may hold values from 0 to 15, as said below
- gate_weights: bfloat16 [4096, 6], P(('grp', 'loc')), may hold values from 0.099609375 to 1
- w_gate: bfloat16 [32, 2048, 704], P(('grp', 'loc')), may hold values from -0.125 to 0.125
- w_up: bfloat16 [32, 2048, 704], P(('grp', 'loc')), may hold values from -0.125 to 0.125
- w_down: bfloat16 [32, 704, 2048], P(('grp', 'loc')), may hold values from -0.15625 to 0.15625
Outputs:
- moe_out: bfloat16 [4096, 2048], P(('grp', 'loc'))
The draws below stay inside these ranges and needn't reach their ends.
Inputs may be any that keep to these rules, and one draw needn't show every extreme that they name: `expert_ids`: each row names 6 different experts in increasing order; they lie in exactly 4 of the 4 groups, expert e belonging to group e // 4.
All inputs are finite; a program needn't handle non-finite values.
Results may differ from the reference program's by a relative error of at most 0.008.
Values may be sent and summed in bfloat16 or wider, within the bound.
A program may use at most 128 MiB of HBM per device.

```python
import math
import jax
import jax.numpy as jnp
from jax import lax

D = 2048
FF = 1408
TOPK = 6
GROUP_LIMIT = 4
TOK_DEV = 128
TOKENS = 4096
EXPERTS = 16
CAP = 72
N_GRP = 4


def draw_expert_ids(key, part):
    group_size = EXPERTS // N_GRP
    key_pop = jax.random.fold_in(key, 11)
    key_grp = jax.random.fold_in(key, 12)
    key_exp = jax.random.fold_in(key, 13)
    popular = jax.random.randint(key_pop, (EXPERTS,), 0, 32768)
    group_score = jax.random.randint(key_grp, (TOKENS, N_GRP), 0, 65536) * N_GRP + jnp.arange(N_GRP, dtype=jnp.int32)[None, :]
    values_top, chosen = lax.top_k(group_score, GROUP_LIMIT)
    chosen_mask = jnp.any(chosen[:, :, None] == jnp.arange(N_GRP, dtype=jnp.int32)[None, None, :], axis=1)
    expert_score = (jax.random.randint(key_exp, (TOKENS, EXPERTS), 0, 65536) + popular[None, :]) * EXPERTS + jnp.arange(EXPERTS, dtype=jnp.int32)[None, :]
    allowed = jnp.repeat(chosen_mask, group_size, axis=1)
    masked = jnp.where(allowed, expert_score, -1)
    by_group = masked.reshape(TOKENS, N_GRP, group_size)
    best_each = jnp.argmax(by_group, axis=2).astype(jnp.int32) + jnp.arange(N_GRP, dtype=jnp.int32)[None, :] * group_size
    picked = jnp.take_along_axis(best_each, chosen, axis=1)
    taken = jnp.any(picked[:, :, None] == jnp.arange(EXPERTS, dtype=jnp.int32)[None, None, :], axis=1)
    remain_score = jnp.where(taken, -1, masked)
    values_more, extra_ids = lax.top_k(remain_score, TOPK - GROUP_LIMIT)
    return jnp.sort(jnp.concatenate([picked, extra_ids.astype(jnp.int32)], axis=1), axis=1).astype(jnp.int32)


def shard_levels(key, dims, shards, smallest, largest):
    loudness, own = 1.0, jax.random.fold_in(key, 6)
    for axis_at, blocks in shards:
        draws = jnp.exp(jax.random.uniform(jax.random.fold_in(own, axis_at), (blocks,), jnp.float32, smallest / len(shards), largest / len(shards)))
        loudness = loudness * jnp.repeat(draws, dims[axis_at] // blocks).reshape([-1 if axis == axis_at else 1 for axis in range(len(dims))])
    return loudness


def scatter_about(rng, dims, width, bound, shards=(), kind=jnp.bfloat16):
    loudness = shard_levels(rng, dims, shards, -0.22, 0.18) if shards else 1.0
    drawn = jax.random.normal(rng, dims, jnp.float32) * width * loudness
    return jnp.minimum(jnp.maximum(drawn, -bound), bound).astype(kind)


def setup_inputs(seed: int = 0) -> dict:
    arg_keys = jax.random.split(jax.random.key(seed), 7)
    tokens = scatter_about(arg_keys[0], (TOKENS, D), 1.0, 6.0, ((0, 32),))
    expert_ids = draw_expert_ids(jax.random.fold_in(arg_keys[6], 71), 0)
    gate_weights = jnp.clip(jnp.exp(math.log(1.0) - 2.306499 * jax.random.uniform(arg_keys[2], (TOKENS, TOPK), jnp.float32) ** shard_levels(arg_keys[2], (TOKENS, TOPK), ((0, 32),), -0.2, 0.2)), 0.099609375, 1.0).astype(jnp.bfloat16)
    w_gate = scatter_about(arg_keys[3], (2 * EXPERTS, D, FF // 2), D ** -0.5, 0.125, ((0, 32),))
    w_up = scatter_about(arg_keys[4], (2 * EXPERTS, D, FF // 2), D ** -0.5, 0.125, ((0, 32),))
    w_down = scatter_about(arg_keys[5], (2 * EXPERTS, FF // 2, D), FF ** -0.5, 0.15625, ((0, 32),))
    return {"tokens": tokens, "expert_ids": expert_ids, "gate_weights": gate_weights, "w_gate": w_gate, "w_up": w_up, "w_down": w_down}


def slot_block(block):
    onehot = (block[:, None] == jnp.arange(EXPERTS, dtype=jnp.int32)[None, :]).astype(jnp.int32)
    before = (jnp.cumsum(onehot, axis=0) - onehot).astype(jnp.int32)
    return jnp.sum(before * onehot, axis=1).astype(jnp.int32)


def reference(tokens, expert_ids, gate_weights, w_gate, w_up, w_down):
    devices = TOKENS // TOK_DEV
    per_group = EXPERTS // N_GRP
    rows_all = devices * CAP
    flat_ids = expert_ids.reshape(devices, TOK_DEV * TOPK)
    slot_of = lax.map(slot_block, flat_ids).reshape(TOKENS, TOPK).astype(jnp.int32)
    is_kept = slot_of < CAP
    token_index = jnp.arange(TOKENS, dtype=jnp.int32)
    row_base = (token_index // TOK_DEV) * CAP
    place_at = jnp.where(is_kept, row_base[:, None] + slot_of, rows_all).astype(jnp.int32)
    weights_kept = jnp.where(is_kept, gate_weights.astype(jnp.float32), jnp.float32(0.0))

    def expert_term(expert):
        matched = expert_ids == expert
        row_of = jnp.sum(jnp.where(matched, place_at, 0), axis=1) + jnp.where(jnp.any(matched, axis=1), 0, rows_all)
        row_of = row_of.astype(jnp.int32)
        weight = jnp.sum(jnp.where(matched, weights_kept, jnp.float32(0.0)), axis=1)
        buffer = jnp.zeros((rows_all + 1, D), jnp.bfloat16).at[row_of].set(tokens)
        summed = jnp.zeros((TOKENS, D), jnp.float32)
        for half_index in range(2):
            weight_row = 2 * expert + half_index
            gate_proj = jnp.dot(buffer, w_gate[weight_row], preferred_element_type=jnp.float32)
            up_proj = jnp.dot(buffer, w_up[weight_row], preferred_element_type=jnp.float32)
            hidden = (jax.nn.silu(gate_proj) * up_proj).astype(jnp.bfloat16)
            half_out = jnp.dot(hidden, w_down[weight_row], preferred_element_type=jnp.float32).astype(jnp.bfloat16)
            summed = summed + half_out[row_of].astype(jnp.float32)
        return weight[:, None] * summed

    def group_step(result, group_id):
        def add_expert(member, accumulated):
            expert = (group_id * per_group + member).astype(jnp.int32)
            return accumulated + expert_term(expert)

        accumulated = lax.fori_loop(0, per_group, add_expert, jnp.zeros((TOKENS, D), jnp.float32))
        rounded = lax.optimization_barrier(accumulated.astype(jnp.bfloat16))
        return result + rounded.astype(jnp.float32), None

    result, ignored = lax.scan(group_step, jnp.zeros((TOKENS, D), jnp.float32), jnp.arange(N_GRP, dtype=jnp.int32))
    return result.astype(jnp.bfloat16)
```

```python
import functools
import jax
import jax.numpy as jnp
from jax import lax
from jax.experimental import pallas as pl
from jax.experimental.pallas import tpu as pltpu
from jax.sharding import PartitionSpec as P


def silu_ffn(row_block, w_gate, w_up, w_down):
    row_shape = row_block.shape
    flat_rows = row_block.reshape(-1, row_shape[-1])
    gate_proj = jnp.dot(flat_rows, w_gate[0], preferred_element_type=jnp.float32)
    up_proj = jnp.dot(flat_rows, w_up[0], preferred_element_type=jnp.float32)
    hidden = (jax.nn.silu(gate_proj) * up_proj).astype(jnp.bfloat16)
    return (
        jnp.dot(hidden, w_down[0], preferred_element_type=jnp.float32)
        .astype(jnp.bfloat16)
        .reshape(row_shape)
    )


def with_zero_row(table):
    return jnp.concatenate([table, jnp.zeros((1, table.shape[1]), table.dtype)], axis=0)


def per_device_slots(tokens, expert_ids, gate_weights, w_gate, w_up, w_down):
    groups = lax.axis_size("grp")
    loc_count = lax.axis_size("loc")
    experts = groups * loc_count // 2
    per_group = loc_count // 2
    tok_count, top_count = expert_ids.shape
    model_width = tokens.shape[1]
    capacity = 3 * tok_count * top_count // (2 * experts)
    flat_ids = expert_ids.reshape(-1)
    onehot = (flat_ids[:, None] == jnp.arange(experts, dtype=jnp.int32)[None, :]).astype(jnp.int32)
    slot_of = jnp.sum((jnp.cumsum(onehot, axis=0) - onehot) * onehot, axis=1).reshape(
        tok_count, top_count
    )
    is_kept = slot_of < capacity
    home_group = expert_ids // per_group
    token_index = jnp.arange(tok_count, dtype=jnp.int32)
    group_range = jnp.arange(groups, dtype=jnp.int32)
    padded = with_zero_row(tokens)
    place_at = jnp.where(is_kept, expert_ids * capacity + slot_of, experts * capacity)
    source_of = (
        jnp.full((experts * capacity + 1,), tok_count, jnp.int32)
        .at[place_at.reshape(-1)]
        .set(jnp.repeat(token_index, top_count))[:-1]
    )
    outgoing = padded[source_of].reshape(experts, 1, capacity, model_width)
    outgoing = jnp.broadcast_to(outgoing, (experts, 2, capacity, model_width)).reshape(
        2 * experts, capacity, model_width
    )
    returned = lax.all_to_all(
        silu_ffn(
            lax.all_to_all(outgoing, ("grp", "loc"), split_axis=0, concat_axis=0, tiled=True),
            w_gate,
            w_up,
            w_down,
        ),
        ("grp", "loc"),
        split_axis=0,
        concat_axis=0,
        tiled=True,
    )
    halves = returned.reshape(experts, 2, capacity, model_width)
    first_half = with_zero_row(halves[:, 0].reshape(-1, model_width))[place_at]
    second_half = with_zero_row(halves[:, 1].reshape(-1, model_width))[place_at]
    weights = jnp.where(is_kept, gate_weights.astype(jnp.float32), jnp.float32(0.0))
    combined = weights[:, :, None] * (
        first_half.astype(jnp.float32) + second_half.astype(jnp.float32)
    )
    group_mask = (home_group[:, :, None] == group_range[None, None, :]).astype(jnp.float32)
    group_sum = jnp.einsum("tkg,tkd->tgd", group_mask, combined, precision=lax.Precision.HIGHEST)
    group_part = lax.optimization_barrier(group_sum.astype(jnp.bfloat16))
    return jnp.sum(group_part.astype(jnp.float32), axis=1).astype(jnp.bfloat16)


MESH = pl.DeviceIdType.MESH
F32 = jnp.float32
BF16 = jnp.bfloat16


def flip(index, bits):
    out, step = index, 1
    while step <= bits:
        if bits & step:
            out = out + step - 2 * step * (lax.rem(index // step, 2))
        step *= 2
    return out


def moe_kernel(
    groups, capacity, tok, info, gate_any, up_any, down_any, out,
    w_gate, w_up, w_down, blocks, infos, rows, peer_out, hid, places, parts,
    sum1, sum2, zsum, send_sem, recv_sem, load_sem,
):
    count, width = tok.shape
    half = width // 2
    padded = places.shape[2]
    a_cols, b_cols = pl.ds(0, half), pl.ds(half, half)
    grp, loc = lax.axis_index("grp"), lax.axis_index("loc")
    expert = (grp * (2 * 4) + loc) // 2
    partner = (grp, flip(loc, 1))

    def peer(k, r):
        return (flip(grp, k), flip(loc, 2 * r))

    others = [(k, r) for k in range(groups) for r in range(4) if k or r]
    barrier = pltpu.get_barrier_semaphore()
    for k, r in others:
        pl.semaphore_signal(barrier, inc=1, device_id=peer(k, r), device_id_type=MESH)
    pl.semaphore_signal(barrier, inc=1, device_id=partner, device_id_type=MESH)

    loads = [
        pltpu.make_async_copy(src.at[0], dst, load_sem.at[i])
        for i, (src, dst) in enumerate(((gate_any, w_gate), (up_any, w_up), (down_any, w_down)))
    ]
    for load in loads:
        load.start()
    pl.semaphore_wait(barrier, len(others) + 1)

    copies = []

    def send(src, dst, device):
        i = len(copies)
        copy = pltpu.make_async_remote_copy(
            src_ref=src, dst_ref=dst, send_sem=send_sem.at[i], recv_sem=recv_sem.at[i],
            device_id=device, device_id_type=MESH,
        )
        copy.start()
        copies.append([copy, False])
        return i

    def got(i):
        copies[i][0].wait_recv()

    def sent(i):
        if not copies[i][1]:
            copies[i][0].wait_send()
            copies[i][1] = True

    info_copy = {kr: send(info, infos.at[kr[0], kr[1]], peer(*kr)) for kr in others}
    z_copy = {}

    def block(k, r):
        return tok if k == 0 and r == 0 else blocks.at[k, r]

    x_copy, y_copy, d_copy, row_copy, out_copy = {}, {}, {}, {}, {}
    a1, b1, a2, b2, zs = {}, {}, {}, {}, {}

    def spread(k):
        if k:
            got(z_copy[k])
        src = block(k, 0)
        x_copy[k, 0] = send(src.at[:, a_cols], blocks.at[k, 1, :, a_cols], peer(0, 1))
        y_copy[k, 1] = send(src.at[:, b_cols], blocks.at[k, 2, :, b_cols], peer(0, 2))
        x_copy[k, 1] = send(src.at[:, b_cols], blocks.at[k, 1, :, b_cols], peer(0, 1))
        y_copy[k, 0] = send(src.at[:, a_cols], blocks.at[k, 2, :, a_cols], peer(0, 2))

    def forward(k):
        got(x_copy[k, 0])
        d_copy[k, 0] = send(blocks.at[k, 1, :, a_cols], blocks.at[k, 3, :, a_cols], peer(0, 2))
        got(y_copy[k, 1])
        d_copy[k, 1] = send(blocks.at[k, 2, :, b_cols], blocks.at[k, 3, :, b_cols], peer(0, 1))

    def pick(k):
        row_at = lax.broadcasted_iota(jnp.int32, (count, count), 0)
        col_at = lax.broadcasted_iota(jnp.int32, (count, count), 1)
        earlier = jnp.where(row_at < col_at, 1.0, 0.0).astype(BF16)
        slot_at = lax.broadcasted_iota(jnp.int32, (padded, count), 0).astype(F32)
        for r in range(4):
            if k or r:
                got(info_copy[k, r])
                table = infos[k, r]
            else:
                table = info[...]
            match = table[:8] == expert.astype(F32)
            used = jnp.sum(jnp.where(match, 1.0, 0.0), axis=0, keepdims=True)
            weight = jnp.sum(jnp.where(match, table[8:], 0.0), axis=0, keepdims=True)
            slot = jnp.dot(
                jnp.broadcast_to(used, (16, count)).astype(BF16), earlier,
                preferred_element_type=F32,
            )[:1]
            slot = jnp.where((used > 0.5) & (slot < capacity), slot, -1.0)
            here = slot_at == jnp.broadcast_to(slot, (padded, count))
            places[k, r] = jnp.where(
                here, jnp.broadcast_to(weight, (padded, count)), 0.0
            ).astype(BF16)
            if r == 1:
                got(x_copy[k, 1])
            if r == 2:
                got(y_copy[k, 0])
            if r == 3:
                got(d_copy[k, 0])
                got(d_copy[k, 1])
            chosen = jnp.where(here, 1.0, 0.0).astype(BF16)
            rows[k, 0, r * padded : (r + 1) * padded, :] = jnp.dot(
                chosen, block(k, r)[...], preferred_element_type=F32
            ).astype(BF16)
        row_copy[k] = send(rows.at[k, 0], rows.at[k, 1], partner)

    def ffn(k, side):
        if side == 0:
            sent(row_copy[k])
        else:
            got(row_copy[k])
        data = rows[k, side]
        gate_proj = jnp.dot(data, w_gate[...], preferred_element_type=F32)
        up_proj = jnp.dot(data, w_up[...], preferred_element_type=F32)
        hid[...] = (gate_proj / (1.0 + jnp.exp(-gate_proj)) * up_proj).astype(BF16)
        tile = width // 4

        @pl.loop(0, 4)
        def _(n):
            cols = pl.ds(pl.multiple_of(n * tile, tile), tile)
            rows[k, side, :, cols] = jnp.dot(
                hid[...], w_down[:, cols], preferred_element_type=F32
            ).astype(BF16)

        if side == 1:
            out_copy[k] = send(rows.at[k, 1], peer_out.at[k], partner)

    def combine(k):
        got(out_copy[k])
        tile = width // 4
        for r in range(4):
            back = places[k, r]
            span = pl.ds(r * padded, padded)

            @pl.loop(0, 4)
            def _(n):
                cols = pl.ds(pl.multiple_of(n * tile, tile), tile)
                total = lax.dot_general(
                    back, rows[k, 0, span, cols], (((0,), (0,)), ((), ())),
                    preferred_element_type=F32,
                ) + lax.dot_general(
                    back, peer_out[k, span, cols], (((0,), (0,)), ((), ())),
                    preferred_element_type=F32,
                )
                parts[k, r, :, cols] = total.astype(BF16)

        a1[k, 2] = send(parts.at[k, 3, :, a_cols], sum1.at[k, 1, :, a_cols], peer(0, 1))
        b1[k, 1] = send(parts.at[k, 3, :, b_cols], sum1.at[k, 1, :, b_cols], peer(0, 2))
        a1[k, 0] = send(parts.at[k, 1, :, a_cols], sum1.at[k, 0, :, a_cols], peer(0, 1))
        b1[k, 0] = send(parts.at[k, 2, :, b_cols], sum1.at[k, 0, :, b_cols], peer(0, 2))

    def add(k, r, cols, other):
        parts[k, r, :, cols] = (
            parts[k, r, :, cols].astype(F32) + other.astype(F32)
        ).astype(BF16)

    def reduce_one(k):
        got(a1[k, 2])
        add(k, 2, a_cols, sum1[k, 1, :, a_cols])
        a2[k] = send(parts.at[k, 2, :, a_cols], sum2.at[k, :, a_cols], peer(0, 2))
        got(b1[k, 1])
        add(k, 1, b_cols, sum1[k, 1, :, b_cols])
        b2[k] = send(parts.at[k, 1, :, b_cols], sum2.at[k, :, b_cols], peer(0, 1))

    def reduce_two(k):
        for first, second, cols in ((a1, a2, a_cols), (b1, b2, b_cols)):
            got(first[k, 0])
            got(second[k])
            add(k, 0, cols, sum1[k, 0, :, cols].astype(F32) + sum2[k, :, cols].astype(F32))
        if k:
            zs[k] = send(parts.at[k, 0], zsum.at[k - 1], peer(k, 0))

    spread(0)
    for k in range(1, groups):
        z_copy[k] = send(tok, blocks.at[k, 0], peer(k, 0))
    spread(1)
    forward(0)
    for k in range(groups):
        pick(k)
        if k == 0:
            for load in loads:
                load.wait()
        ffn(k, 0)
        if k + 1 < groups:
            forward(k + 1)
        ffn(k, 1)
        if k + 2 < groups:
            spread(k + 2)
        if k >= 1:
            reduce_one(k - 1)
        if k >= 2:
            reduce_two(k - 2)
        combine(k)
    if groups >= 2:
        reduce_two(groups - 2)
    reduce_one(groups - 1)
    reduce_two(groups - 1)
    total = parts[0, 0].astype(F32)
    for k in range(1, groups):
        got(zs[k])
        total = total + zsum[k - 1].astype(F32)
    out[...] = total.astype(out.dtype)
    for i in range(len(copies)):
        sent(i)


def per_device_direct(tokens, expert_ids, gate_weights, w_gate, w_up, w_down):
    groups = lax.axis_size("grp")
    experts = groups * lax.axis_size("loc") // 2
    count, top_count = expert_ids.shape
    width, units = w_gate.shape[1:]
    capacity = 3 * count * top_count // (2 * experts)
    padded = -(-capacity // 16) * 16
    info = jnp.concatenate(
        [
            jnp.pad(expert_ids.T.astype(F32), ((0, 8 - top_count), (0, 0)), constant_values=-1.0),
            jnp.pad(gate_weights.T.astype(F32), ((0, 8 - top_count), (0, 0))),
        ],
        axis=0,
    )
    copies = groups * 4 - 1 + groups - 1 + groups * 14 + groups - 1
    vmem = pl.BlockSpec(memory_space=pltpu.VMEM)
    hbm = pl.BlockSpec(memory_space=pl.ANY)
    return pl.pallas_call(
        functools.partial(moe_kernel, groups, capacity),
        out_shape=jax.ShapeDtypeStruct((count, width), tokens.dtype),
        in_specs=[vmem, vmem, hbm, hbm, hbm],
        out_specs=vmem,
        scratch_shapes=[
            pltpu.VMEM((width, units), BF16),
            pltpu.VMEM((width, units), BF16),
            pltpu.VMEM((units, width), BF16),
            pltpu.VMEM((groups, 4, count, width), BF16),
            pltpu.VMEM((groups, 4, 16, count), F32),
            pltpu.VMEM((groups, 2, 4 * padded, width), BF16),
            pltpu.VMEM((groups, 4 * padded, width), BF16),
            pltpu.VMEM((4 * padded, units), BF16),
            pltpu.VMEM((groups, 4, padded, count), BF16),
            pltpu.VMEM((groups, 4, count, width), BF16),
            pltpu.VMEM((groups, 2, count, width), BF16),
            pltpu.VMEM((groups, count, width), BF16),
            pltpu.VMEM((groups - 1, count, width), BF16),
            pltpu.SemaphoreType.DMA((copies,)),
            pltpu.SemaphoreType.DMA((copies,)),
            pltpu.SemaphoreType.DMA((3,)),
        ],
        compiler_params=pltpu.CompilerParams(
            collective_id=0, has_side_effects=True, vmem_limit_bytes=67043328
        ),
    )(tokens, info, w_gate, w_up, w_down)


def solution(mesh):
    groups, locs = mesh.shape["grp"], mesh.shape["loc"]
    direct = locs == 8 and groups in (2, 4)
    spec = P(("grp", "loc"), None)
    wide = P(("grp", "loc"), None, None)
    return jax.shard_map(
        per_device_direct if direct else per_device_slots,
        mesh=mesh,
        in_specs=(spec, spec, spec, wide, wide, wide),
        out_specs=spec,
        check_vma=False,
    )
```

```python
import functools
import jax
import jax.numpy as jnp
from jax import lax
from jax.experimental import pallas as pl
from jax.experimental.pallas import tpu as pltpu
from jax.sharding import PartitionSpec as P


def silu_ffn(row_block, w_gate, w_up, w_down):
    row_shape = row_block.shape
    flat_rows = row_block.reshape(-1, row_shape[-1])
    gate_proj = jnp.dot(flat_rows, w_gate[0], preferred_element_type=jnp.float32)
    up_proj = jnp.dot(flat_rows, w_up[0], preferred_element_type=jnp.float32)
    hidden = (jax.nn.silu(gate_proj) * up_proj).astype(jnp.bfloat16)
    return (
        jnp.dot(hidden, w_down[0], preferred_element_type=jnp.float32)
        .astype(jnp.bfloat16)
        .reshape(row_shape)
    )


def with_zero_row(table):
    return jnp.concatenate([table, jnp.zeros((1, table.shape[1]), table.dtype)], axis=0)


def per_device_slots(tokens, expert_ids, gate_weights, w_gate, w_up, w_down):
    groups = lax.axis_size("grp")
    loc_count = lax.axis_size("loc")
    experts = groups * loc_count // 2
    per_group = loc_count // 2
    tok_count, top_count = expert_ids.shape
    model_width = tokens.shape[1]
    capacity = 3 * tok_count * top_count // (2 * experts)
    flat_ids = expert_ids.reshape(-1)
    onehot = (flat_ids[:, None] == jnp.arange(experts, dtype=jnp.int32)[None, :]).astype(jnp.int32)
    slot_of = jnp.sum((jnp.cumsum(onehot, axis=0) - onehot) * onehot, axis=1).reshape(
        tok_count, top_count
    )
    is_kept = slot_of < capacity
    home_group = expert_ids // per_group
    token_index = jnp.arange(tok_count, dtype=jnp.int32)
    group_range = jnp.arange(groups, dtype=jnp.int32)
    padded = with_zero_row(tokens)
    place_at = jnp.where(is_kept, expert_ids * capacity + slot_of, experts * capacity)
    source_of = (
        jnp.full((experts * capacity + 1,), tok_count, jnp.int32)
        .at[place_at.reshape(-1)]
        .set(jnp.repeat(token_index, top_count))[:-1]
    )
    outgoing = padded[source_of].reshape(experts, 1, capacity, model_width)
    outgoing = jnp.broadcast_to(outgoing, (experts, 2, capacity, model_width)).reshape(
        2 * experts, capacity, model_width
    )
    returned = lax.all_to_all(
        silu_ffn(
            lax.all_to_all(outgoing, ("grp", "loc"), split_axis=0, concat_axis=0, tiled=True),
            w_gate,
            w_up,
            w_down,
        ),
        ("grp", "loc"),
        split_axis=0,
        concat_axis=0,
        tiled=True,
    )
    halves = returned.reshape(experts, 2, capacity, model_width)
    first_half = with_zero_row(halves[:, 0].reshape(-1, model_width))[place_at]
    second_half = with_zero_row(halves[:, 1].reshape(-1, model_width))[place_at]
    weights = jnp.where(is_kept, gate_weights.astype(jnp.float32), jnp.float32(0.0))
    combined = weights[:, :, None] * (
        first_half.astype(jnp.float32) + second_half.astype(jnp.float32)
    )
    group_mask = (home_group[:, :, None] == group_range[None, None, :]).astype(jnp.float32)
    group_sum = jnp.einsum("tkg,tkd->tgd", group_mask, combined, precision=lax.Precision.HIGHEST)
    group_part = lax.optimization_barrier(group_sum.astype(jnp.bfloat16))
    return jnp.sum(group_part.astype(jnp.float32), axis=1).astype(jnp.bfloat16)


MESH = pl.DeviceIdType.MESH
F32 = jnp.float32
BF16 = jnp.bfloat16


def flip(index, bits):
    out, step = index, 1
    while step <= bits:
        if bits & step:
            out = out + step - 2 * step * (lax.rem(index // step, 2))
        step *= 2
    return out


def moe_kernel(
    groups, capacity, tok, info, gate_any, up_any, down_any, out,
    w_gate, w_up, w_down, blocks, infos, rows, peer_out, hid, places, parts,
    sum1, sum2, zsum, send_sem, recv_sem, load_sem,
):
    count, width = tok.shape
    half = width // 2
    padded = places.shape[2]
    a_cols, b_cols = pl.ds(0, half), pl.ds(half, half)
    grp, loc = lax.axis_index("grp"), lax.axis_index("loc")
    expert = (grp * (2 * 4) + loc) // 2
    partner = (grp, flip(loc, 1))

    def peer(k, r):
        return (flip(grp, k), flip(loc, 2 * r))

    others = [(k, r) for k in range(groups) for r in range(4) if k or r]
    barrier = pltpu.get_barrier_semaphore()
    for k, r in others:
        pl.semaphore_signal(barrier, inc=1, device_id=peer(k, r), device_id_type=MESH)
    pl.semaphore_signal(barrier, inc=1, device_id=partner, device_id_type=MESH)

    loads = [
        pltpu.make_async_copy(src.at[0], dst, load_sem.at[i])
        for i, (src, dst) in enumerate(((gate_any, w_gate), (up_any, w_up), (down_any, w_down)))
    ]
    for load in loads:
        load.start()
    pl.semaphore_wait(barrier, len(others) + 1)

    copies = []

    def send(src, dst, device):
        i = len(copies)
        copy = pltpu.make_async_remote_copy(
            src_ref=src, dst_ref=dst, send_sem=send_sem.at[i], recv_sem=recv_sem.at[i],
            device_id=device, device_id_type=MESH,
        )
        copy.start()
        copies.append([copy, False])
        return i

    def got(i):
        copies[i][0].wait_recv()

    def sent(i):
        if not copies[i][1]:
            copies[i][0].wait_send()
            copies[i][1] = True

    info_copy = {kr: send(info, infos.at[kr[0], kr[1]], peer(*kr)) for kr in others}
    z_copy = {}

    def block(k, r):
        return tok if k == 0 and r == 0 else blocks.at[k, r]

    x_copy, y_copy, d_copy, row_copy, out_copy = {}, {}, {}, {}, {}
    a1, b1, a2, b2, zs = {}, {}, {}, {}, {}

    def spread(k):
        if k:
            got(z_copy[k])
        src = block(k, 0)
        x_copy[k, 0] = send(src.at[:, a_cols], blocks.at[k, 1, :, a_cols], peer(0, 1))
        y_copy[k, 1] = send(src.at[:, b_cols], blocks.at[k, 2, :, b_cols], peer(0, 2))
        x_copy[k, 1] = send(src.at[:, b_cols], blocks.at[k, 1, :, b_cols], peer(0, 1))
        y_copy[k, 0] = send(src.at[:, a_cols], blocks.at[k, 2, :, a_cols], peer(0, 2))

    def forward(k):
        got(x_copy[k, 0])
        d_copy[k, 0] = send(blocks.at[k, 1, :, a_cols], blocks.at[k, 3, :, a_cols], peer(0, 2))
        got(y_copy[k, 1])
        d_copy[k, 1] = send(blocks.at[k, 2, :, b_cols], blocks.at[k, 3, :, b_cols], peer(0, 1))

    def pick(k):
        row_at = lax.broadcasted_iota(jnp.int32, (count, count), 0)
        col_at = lax.broadcasted_iota(jnp.int32, (count, count), 1)
        earlier = jnp.where(row_at < col_at, 1.0, 0.0).astype(BF16)
        slot_at = lax.broadcasted_iota(jnp.int32, (padded, count), 0).astype(F32)
        for r in range(4):
            if k or r:
                got(info_copy[k, r])
                table = infos[k, r]
            else:
                table = info[...]
            match = table[:8] == expert.astype(F32)
            used = jnp.sum(jnp.where(match, 1.0, 0.0), axis=0, keepdims=True)
            weight = jnp.sum(jnp.where(match, table[8:], 0.0), axis=0, keepdims=True)
            slot = jnp.dot(
                jnp.broadcast_to(used, (16, count)).astype(BF16), earlier,
                preferred_element_type=F32,
            )[:1]
            slot = jnp.where((used > 0.5) & (slot < capacity), slot, -1.0)
            here = slot_at == jnp.broadcast_to(slot, (padded, count))
            places[k, r] = jnp.where(
                here, jnp.broadcast_to(weight, (padded, count)), 0.0
            ).astype(BF16)
            if r == 1:
                got(x_copy[k, 1])
            if r == 2:
                got(y_copy[k, 0])
            if r == 3:
                got(d_copy[k, 0])
                got(d_copy[k, 1])
            chosen = jnp.where(here, 1.0, 0.0).astype(BF16)
            rows[k, 0, r * padded : (r + 1) * padded, :] = jnp.dot(
                chosen, block(k, r)[...], preferred_element_type=F32
            ).astype(BF16)
        row_copy[k] = send(rows.at[k, 0], rows.at[k, 1], partner)

    def ffn(k, side):
        if side == 0:
            sent(row_copy[k])
        else:
            got(row_copy[k])
        data = rows[k, side]
        gate_proj = jnp.dot(data, w_gate[...], preferred_element_type=F32)
        up_proj = jnp.dot(data, w_up[...], preferred_element_type=F32)
        hid[...] = (gate_proj / (1.0 + jnp.exp(-gate_proj)) * up_proj).astype(BF16)
        tile = width // 4

        @pl.loop(0, 4)
        def _(n):
            cols = pl.ds(pl.multiple_of(n * tile, tile), tile)
            rows[k, side, :, cols] = jnp.dot(
                hid[...], w_down[:, cols], preferred_element_type=F32
            ).astype(BF16)

        if side == 1:
            out_copy[k] = send(rows.at[k, 1], peer_out.at[k], partner)

    def combine(k):
        got(out_copy[k])
        tile = width // 4
        for r in (3, 1, 2, 0):
            back = places[k, r]
            span = pl.ds(r * padded, padded)

            @pl.loop(0, 4)
            def _(n):
                cols = pl.ds(pl.multiple_of(n * tile, tile), tile)
                total = lax.dot_general(
                    back, rows[k, 0, span, cols], (((0,), (0,)), ((), ())),
                    preferred_element_type=F32,
                ) + lax.dot_general(
                    back, peer_out[k, span, cols], (((0,), (0,)), ((), ())),
                    preferred_element_type=F32,
                )
                parts[k, r, :, cols] = total.astype(BF16)

            if r & 1:
                a1[k, r - 1] = send(
                    parts.at[k, r, :, a_cols], sum1.at[k, r // 2, :, a_cols], peer(0, 1)
                )
            if r & 2:
                b1[k, r - 2] = send(
                    parts.at[k, r, :, b_cols], sum1.at[k, r - 2, :, b_cols], peer(0, 2)
                )

    def add(k, r, cols, other):
        parts[k, r, :, cols] = (
            parts[k, r, :, cols].astype(F32) + other.astype(F32)
        ).astype(BF16)

    def reduce_one(k):
        got(a1[k, 2])
        add(k, 2, a_cols, sum1[k, 1, :, a_cols])
        a2[k] = send(parts.at[k, 2, :, a_cols], sum2.at[k, :, a_cols], peer(0, 2))
        got(b1[k, 1])
        add(k, 1, b_cols, sum1[k, 1, :, b_cols])
        b2[k] = send(parts.at[k, 1, :, b_cols], sum2.at[k, :, b_cols], peer(0, 1))

    def reduce_two(k):
        for first, second, cols in ((a1, a2, a_cols), (b1, b2, b_cols)):
            got(first[k, 0])
            got(second[k])
            add(k, 0, cols, sum1[k, 0, :, cols].astype(F32) + sum2[k, :, cols].astype(F32))
        if k:
            zs[k] = send(parts.at[k, 0], zsum.at[k - 1], peer(k, 0))

    spread(0)
    for k in range(1, groups):
        z_copy[k] = send(tok, blocks.at[k, 0], peer(k, 0))
    forward(0)
    spread(1)
    for k in range(groups):
        pick(k)
        if k == 0:
            for load in loads:
                load.wait()
        ffn(k, 0)
        if k + 1 < groups:
            forward(k + 1)
        if k >= 3:
            reduce_two(k - 2)
        ffn(k, 1)
        if k + 2 < groups:
            spread(k + 2)
        if k >= 2:
            reduce_one(k - 1)
        if k >= 1:
            combine(k)
    combine(0)
    if groups >= 3:
        reduce_two(groups - 2)
    reduce_one(groups - 1)
    reduce_one(0)
    reduce_two(groups - 1)
    reduce_two(0)
    total = parts[0, 0].astype(F32)
    for k in range(1, groups):
        got(zs[k])
        total = total + zsum[k - 1].astype(F32)
    out[...] = total.astype(out.dtype)
    for i in range(len(copies)):
        sent(i)


def per_device_direct(tokens, expert_ids, gate_weights, w_gate, w_up, w_down):
    groups = lax.axis_size("grp")
    experts = groups * lax.axis_size("loc") // 2
    count, top_count = expert_ids.shape
    width, units = w_gate.shape[1:]
    capacity = 3 * count * top_count // (2 * experts)
    padded = -(-capacity // 16) * 16
    info = jnp.concatenate(
        [
            jnp.pad(expert_ids.T.astype(F32), ((0, 8 - top_count), (0, 0)), constant_values=-1.0),
            jnp.pad(gate_weights.T.astype(F32), ((0, 8 - top_count), (0, 0))),
        ],
        axis=0,
    )
    copies = groups * 4 - 1 + groups - 1 + groups * 14 + groups - 1
    vmem = pl.BlockSpec(memory_space=pltpu.VMEM)
    hbm = pl.BlockSpec(memory_space=pl.ANY)
    return pl.pallas_call(
        functools.partial(moe_kernel, groups, capacity),
        out_shape=jax.ShapeDtypeStruct((count, width), tokens.dtype),
        in_specs=[vmem, vmem, hbm, hbm, hbm],
        out_specs=vmem,
        scratch_shapes=[
            pltpu.VMEM((width, units), BF16),
            pltpu.VMEM((width, units), BF16),
            pltpu.VMEM((units, width), BF16),
            pltpu.VMEM((groups, 4, count, width), BF16),
            pltpu.VMEM((groups, 4, 16, count), F32),
            pltpu.VMEM((groups, 2, 4 * padded, width), BF16),
            pltpu.VMEM((groups, 4 * padded, width), BF16),
            pltpu.VMEM((4 * padded, units), BF16),
            pltpu.VMEM((groups, 4, padded, count), BF16),
            pltpu.VMEM((groups, 4, count, width), BF16),
            pltpu.VMEM((groups, 2, count, width), BF16),
            pltpu.VMEM((groups, count, width), BF16),
            pltpu.VMEM((groups - 1, count, width), BF16),
            pltpu.SemaphoreType.DMA((copies,)),
            pltpu.SemaphoreType.DMA((copies,)),
            pltpu.SemaphoreType.DMA((3,)),
        ],
        compiler_params=pltpu.CompilerParams(
            collective_id=0, has_side_effects=True, vmem_limit_bytes=67043328
        ),
    )(tokens, info, w_gate, w_up, w_down)


def solution(mesh):
    groups, locs = mesh.shape["grp"], mesh.shape["loc"]
    direct = locs == 8 and groups in (2, 4)
    spec = P(("grp", "loc"), None)
    wide = P(("grp", "loc"), None, None)
    return jax.shard_map(
        per_device_direct if direct else per_device_slots,
        mesh=mesh,
        in_specs=(spec, spec, spec, wide, wide, wide),
        out_specs=spec,
        check_vma=False,
    )
```
